32 devices in a mesh: sub: 4 (over z), ma: 8 (over y, x, core).
Axes of the slice: x: 2, y: 2, z: 4, core: 2. Of those that a mesh axis runs over, the one named last changes fastest.
Arguments:
- forcing: float32 [2, 256, 2, 64, 512], P(None, 'sub', None, 'ma'), may hold values from -24 to 24
- slot_wavenumber: int32 [64], P('ma'), may hold values from 0 to 511, as said below
- inverse: float32 [4, 2, 64, 64, 512], P('sub'), may hold values from -2 to 2
- edge_weights: float32 [4, 2, 64], P('sub'), may hold values from -1357 to 1357, as said below
Outputs:
- transform_field: float32 [2, 256, 2, 64, 512], P(None, ('sub', 'ma'))
The draws below stay inside these ranges and needn't reach their ends.
Inputs may be any that keep to these rules, and one draw needn't show every extreme that they name: `slot_wavenumber`: each device's slots hold 4 pairs: slots 2j and 2j + 1 carry a wavenumber m below 256 and 511 - m, in that order; no wavenumber appears twice. `edge_weights`: together with inverse it makes every row of the interface system strictly diagonally dominant with a positive diagonal.
All inputs are finite; a program needn't handle non-finite values.
Results may differ from the reference program's by a relative error of at most 0.0003.
Values sent between devices are 32-bit elements; how exact they have to be, the bound alone decides.
A program may use at most 192 MiB of HBM per device.

```python
import math
import jax
import jax.numpy as jnp
from jax import lax

P_SIZE = 64
L = 512
FIELDS = 2
NSUB = 4
MTOT = 64
NR = 256


def shell_radius(key):
    widths = jax.random.uniform(jax.random.fold_in(key, 11), (NSUB,), jnp.float32, 1.0, 2.0)
    widths = 0.65 * widths / jnp.sum(widths)
    starts = 0.35 + jnp.cumsum(widths) - widths
    spacing = jnp.arange(P_SIZE, dtype=jnp.float32) / (P_SIZE - 1)
    return (starts[:, None] + widths[:, None] * spacing[None, :], widths)


def draw_slot_wavenumber(key, part):
    halfway = L // 2
    chosen = jax.random.permutation(jax.random.fold_in(key, 21), halfway)[:MTOT // 2]
    paired = jnp.stack([chosen, L - 1 - chosen], axis=1).reshape(MTOT)
    return paired.astype(jnp.int32)


def draw_edge_weights(key, part):
    radius, widths = shell_radius(key)
    step_size = widths / (P_SIZE - 1)
    lower_row = jnp.zeros((NSUB, P_SIZE), jnp.float32)
    lower_row = lower_row.at[:, 0].set(-1.5 / step_size).at[:, 1].set(2.0 / step_size).at[:, 2].set(-0.5 / step_size)
    upper_row = jnp.zeros((NSUB, P_SIZE), jnp.float32)
    upper_row = upper_row.at[:, P_SIZE - 1].set(1.5 / step_size).at[:, P_SIZE - 2].set(-2.0 / step_size).at[:, P_SIZE - 3].set(0.5 / step_size)
    return jnp.stack([lower_row, upper_row], axis=1)


def draw_inverse(key, part):
    radius, widths = shell_radius(key)
    field_scale = jnp.exp(jax.random.uniform(jax.random.fold_in(key, 12), (FIELDS,), jnp.float32, math.log(0.05), math.log(0.5)))
    degree_scale = jnp.exp(jax.random.uniform(jax.random.fold_in(key, 13), (FIELDS, L), jnp.float32, 0.0, math.log(3.0)))
    strength = (field_scale[:, None] * degree_scale)[None, :, :, None]
    degree = jnp.arange(L, dtype=jnp.float32)
    angular = degree * (degree + 1.0)
    inner = radius[:, 1:-1]
    below_gap = radius[:, 1:-1] - radius[:, :-2]
    above_gap = radius[:, 2:] - radius[:, 1:-1]
    spans = below_gap + above_gap
    sub_coef = 2.0 / (below_gap * spans) - 2.0 / (inner * spans)
    sup_coef = 2.0 / (above_gap * spans) + 2.0 / (inner * spans)
    mid_coef = 2.0 / (below_gap * above_gap)
    lower_band = -strength * sub_coef[:, None, None, :]
    upper_band = -strength * sup_coef[:, None, None, :]
    main_band = 1.0 + strength * (mid_coef[:, None, None, :] + angular[None, None, :, None] / (inner[:, None, None, :] * inner[:, None, None, :]))
    edges = ((0, 0), (0, 0), (0, 0), (1, 1))
    lower_band = jnp.pad(lower_band, edges)
    upper_band = jnp.pad(upper_band, edges)
    main_band = jnp.pad(main_band, edges, constant_values=1.0)
    bands = (jnp.moveaxis(lower_band, -1, 0), jnp.moveaxis(main_band, -1, 0), jnp.moveaxis(upper_band, -1, 0), jnp.eye(P_SIZE, dtype=jnp.float32))

    def forward(state_pair, inputs):
        prior_ratio, prior_value = state_pair
        sub_entry, main_entry, sup_entry, unit_row = inputs
        pivot_value = main_entry - sub_entry * prior_ratio
        ratio_next = sup_entry / pivot_value
        value_next = (unit_row[None, None, None, :] - sub_entry[..., None] * prior_value) / pivot_value[..., None]
        return ((ratio_next, value_next), (ratio_next, value_next))
    initial = (jnp.zeros((NSUB, FIELDS, L), jnp.float32), jnp.zeros((NSUB, FIELDS, L, P_SIZE), jnp.float32))
    _, (ratios, values) = lax.scan(forward, initial, bands)

    def backward(later_value, inputs):
        ratio_here, value_here = inputs
        current = value_here - ratio_here[..., None] * later_value
        return (current, current)
    _, solved = lax.scan(backward, jnp.zeros((NSUB, FIELDS, L, P_SIZE), jnp.float32), (ratios, values), reverse=True)
    position = jnp.arange(P_SIZE)
    interior = ((position > 0) & (position < P_SIZE - 1)).astype(jnp.float32)
    noise = jax.random.truncated_normal(jax.random.fold_in(key, 14), -3.0, 3.0, (NSUB, FIELDS, P_SIZE, P_SIZE, L), jnp.float32)
    inner_mask = (interior[:, None] * interior[None, :])[None, None, :, :, None]
    mixing = jnp.eye(P_SIZE, dtype=jnp.float32)[None, None, :, :, None] + 0.5 * noise / math.sqrt(P_SIZE - 2) * inner_mask
    return jnp.einsum('isflk,sfkjl->sfijl', solved, mixing, precision=lax.Precision.HIGHEST)


def block_levels(rng, dims, split, smallest, largest):
    def one(dim, blocks):
        draws = jax.random.uniform(jax.random.fold_in(jax.random.fold_in(rng, 6), dim), (blocks,), jnp.float32, smallest / len(split), largest / len(split))
        return jnp.repeat(jnp.exp(draws), dims[dim] // blocks).reshape((-1,) + (1,) * (len(dims) - dim - 1))

    loudness = one(*split[0])
    for cut in split[1:]:
        loudness = loudness * one(*cut)
    return loudness


def scatter_about(key, shape, scale, most, split=(), held_as=jnp.bfloat16):
    drawn = scale * jax.random.normal(key, shape, jnp.float32)
    if split:
        drawn = drawn * block_levels(key, shape, split, -0.22, 0.18)
    return jnp.clip(drawn, -most, most).astype(held_as)


def setup_inputs(seed: int = 0) -> dict:
    arg_keys = jax.random.split(jax.random.key(seed), 5)
    forcing = scatter_about(arg_keys[0], (FIELDS, NR, 2, MTOT, L), 4.0, 24.0, ((1, 4), (3, 8)), jnp.float32)
    slot_wavenumber = draw_slot_wavenumber(jax.random.fold_in(arg_keys[4], 71), 0)
    inverse = draw_inverse(jax.random.fold_in(arg_keys[4], 71), 0)
    edge_weights = draw_edge_weights(jax.random.fold_in(arg_keys[4], 71), 0)
    return {"forcing": forcing, "slot_wavenumber": slot_wavenumber, "inverse": inverse, "edge_weights": edge_weights}


HIGH = lax.Precision.HIGHEST


def local_solve(pair):
    block_inverse, block_source = pair
    return jnp.einsum('fpql,fqcml->fpcml', block_inverse, block_source, precision=HIGH)


def reference(forcing, slot_wavenumber, inverse, edge_weights):
    degree = jnp.arange(L, dtype=jnp.int32)
    kept_modes = (degree[None, :] >= slot_wavenumber[:, None]).astype(jnp.float32)
    position = jnp.arange(P_SIZE, dtype=jnp.int32)
    interior = ((position > 0) & (position < P_SIZE - 1)).astype(jnp.float32)
    source = forcing.reshape(FIELDS, NSUB, P_SIZE, 2, MTOT, L)
    source = source * kept_modes[None, None, None, None, :, :] * interior[None, None, :, None, None, None]
    source = jnp.transpose(source, (1, 0, 2, 3, 4, 5))
    particular = lax.map(local_solve, (inverse, source))
    low_row = edge_weights[:, 0, :]
    top_row = edge_weights[:, 1, :]
    low_slope = jnp.einsum('sp,sfpcml->sfcml', low_row, particular, precision=HIGH)
    top_slope = jnp.einsum('sp,sfpcml->sfcml', top_row, particular, precision=HIGH)
    lower_unit = inverse[:, :, :, 0, :]
    upper_unit = inverse[:, :, :, P_SIZE - 1, :]
    low_lower = jnp.einsum('sp,sfpl->sfl', low_row, lower_unit, precision=HIGH)
    low_upper = jnp.einsum('sp,sfpl->sfl', low_row, upper_unit, precision=HIGH)
    top_lower = jnp.einsum('sp,sfpl->sfl', top_row, lower_unit, precision=HIGH)
    top_upper = jnp.einsum('sp,sfpl->sfl', top_row, upper_unit, precision=HIGH)
    ratio_now = jnp.zeros((FIELDS, L), jnp.float32)
    reduced = jnp.zeros((FIELDS, 2, MTOT, L), jnp.float32)
    ratio_list = []
    reduced_list = []
    for level in range(NSUB - 1):
        lower_coef = top_lower[level]
        middle_coef = top_upper[level] - low_lower[level + 1]
        upper_coef = -low_upper[level + 1]
        right_side = low_slope[level + 1] - top_slope[level]
        pivot_value = middle_coef - lower_coef * ratio_now
        ratio_now = upper_coef / pivot_value
        reduced = (right_side - lower_coef[:, None, None, :] * reduced) / pivot_value[:, None, None, :]
        ratio_list.append(ratio_now)
        reduced_list.append(reduced)
    later_value = jnp.zeros((FIELDS, 2, MTOT, L), jnp.float32)
    interface = [later_value] * (NSUB - 1)
    for level in range(NSUB - 2, -1, -1):
        later_value = reduced_list[level] - ratio_list[level][:, None, None, :] * later_value
        interface[level] = later_value
    boundary = jnp.zeros((FIELDS, 2, MTOT, L), jnp.float32)
    lower_value = jnp.stack([boundary] + interface)
    upper_value = jnp.stack(interface + [boundary])
    solution = particular + lower_value[:, :, None] * lower_unit[:, :, :, None, None, :]
    solution = solution + upper_value[:, :, None] * upper_unit[:, :, :, None, None, :]
    return jnp.transpose(solution, (1, 0, 2, 3, 4, 5)).reshape(FIELDS, NR, 2, MTOT, L)
```

```python
import functools

import jax
import jax.numpy as jnp
from jax import lax
from jax.experimental import pallas as pl
from jax.experimental.pallas import tpu as pltpu
from jax.sharding import PartitionSpec as P

LANES = 128
ROWS = 8
F32 = jnp.float32
MESH = pl.DeviceIdType.MESH


def grid_iotas():
    row = lax.broadcasted_iota(jnp.int32, (ROWS, LANES), 0)
    lane = lax.broadcasted_iota(jnp.int32, (ROWS, LANES), 1)
    return row, lane


def lane_gather(values, index):
    return jnp.take_along_axis(values, index, axis=1, mode="promise_in_bounds")


def solve_kernel(
    dims, slot, edge, forcing, inverse, packed, ends, cols, even_src, odd_src, part, edge_sum
):
    fields, points, degrees, group = dims
    tiles = degrees // LANES
    half = tiles // 2
    wide = tiles + half
    blocks = points // ROWS
    g = pl.program_id(0)
    row, lane = grid_iotas()
    is_even = (row & 1) == 0
    m = jnp.zeros((ROWS, LANES), jnp.int32)
    for j in range(ROWS // 2):
        m = jnp.where((row >> 1) == j, slot[2 * j], m)

    @pl.when(g == 0)
    def _():
        ends[...] = jnp.zeros_like(ends)
        edge_sum[...] = jnp.zeros_like(edge_sum)

        def prepare(q, _):
            inside = jnp.where((q > 0) & (q < points - 1), 1.0, 0.0).astype(F32)
            for f in range(fields):
                for t in range(tiles):
                    at = pl.ds(t * LANES, LANES)
                    a = forcing[f, q, 0, :, at] * inside
                    b = forcing[f, q, 1, :, at] * inside
                    degree = lane + t * LANES
                    mixed = jnp.where(is_even, a, pltpu.roll(b, 1, 0))
                    even_src[f, q, t] = jnp.where(degree >= m, mixed, 0.0)
                    if t >= half:
                        mixed = jnp.where(is_even, pltpu.roll(a, ROWS - 1, 0), b)
                        odd_src[f, q, t - half] = jnp.where(degree >= degrees - 1 - m, mixed, 0.0)
            return 0

        lax.fori_loop(0, points, prepare, 0)

    shift_index = (lane - m) & (LANES - 1)
    left_index = (degrees - 1 - m) & (LANES - 1)
    left = jnp.zeros((ROWS, LANES), F32)
    for f in range(fields):
        weights = [[edge[0, e, g * group + p] for p in range(group)] for e in range(2)]
        for t in range(tiles):
            at = pl.ds(t * LANES, LANES)
            both = t >= half

            def step(block, sums, f=f, t=t, at=at, both=both):
                sums = list(sums)
                for i in range(ROWS):
                    q = block * ROWS + i
                    even = even_src[f, q, t]
                    odd = odd_src[f, q, t - half] if both else None
                    for p in range(group):
                        line = inverse[0, f, p, block, pl.ds(i, 1), at]
                        entry = jnp.broadcast_to(line, (ROWS, LANES))
                        sums[p] += entry * even
                        if both:
                            sums[group + p] += entry * odd
                return tuple(sums)

            start = tuple(jnp.zeros((ROWS, LANES), F32) for _ in range(group * (2 if both else 1)))
            sums = lax.fori_loop(0, blocks, step, start)
            for p in range(group):
                part[p, t] = sums[p]
                if both:
                    part[p, tiles + t - half] = sums[group + p]
            for e in range(2):
                base = (e * fields + f) * wide
                ends[base + t] += sum(weights[e][p] * sums[p] for p in range(group))
                if both:
                    ends[base + tiles + t - half] += sum(
                        weights[e][p] * sums[group + p] for p in range(group)
                    )
                for w in range(2):
                    edge_block = w * (blocks - 1)
                    edge_sum[e, f, w, t] += sum(
                        weights[e][p] * inverse[0, f, p, edge_block, :, at] for p in range(group)
                    )
        for p in range(group):
            k = f * group + p
            near, far = part[p, tiles], part[p, tiles + 1]
            near_moved = lane_gather(near, shift_index)
            far_moved = lane_gather(far, shift_index)
            packed[0, k * tiles] = jnp.where(
                lane >= m, part[p, 0], jnp.where(lane - m >= -LANES, far_moved, near_moved)
            )
            packed[0, k * tiles + 1] = jnp.where(lane + LANES >= m, part[p, 1], far_moved)
            packed[0, k * tiles + 2] = part[p, 2]
            packed[0, k * tiles + 3] = part[p, 3]
            spare = jnp.where(
                m < LANES, lane_gather(far, left_index), lane_gather(near, left_index)
            )
            left = jnp.where(lane == k, spare, left)
    packed[0, fields * group * tiles] = left
    packed[0, fields * group * tiles + 1] = m.astype(F32)

    @pl.when(g == lax.axis_index("ma"))
    def _():
        for f in range(fields):
            for p in range(group):
                cols[0, f, pl.ds(p, 1), :] = inverse[0, f, p, 0, pl.ds(0, 1), :]
                cols[1, f, pl.ds(p, 1), :] = inverse[0, f, p, blocks - 1, pl.ds(ROWS - 1, 1), :]

    @pl.when(g == pl.num_programs(0) - 1)
    def _():
        base = 2 * fields * wide
        for f in range(fields):
            for e in range(2):
                for w in range(2):
                    at = f * 4 + e * 2 + w
                    for t in range(wide):
                        source = t if t < tiles else t - half
                        line = edge_sum[e, f, w, source, pl.ds(w * (ROWS - 1), 1), :]
                        ends[base + t, pl.ds(at, 1), :] = line


def exchange_kernel(
    dims, packed, ends, landed, values_landed,
    everyone, values, z_send, z_recv, p_send, p_recv, u_send, u_recv, own_sem,
):
    fields, wide, subs, groups = dims
    sub = lax.axis_index("sub")
    me = lax.axis_index("ma")
    subs_to = [lax.rem(sub + k, subs) for k in range(1, subs)]
    groups_to = [lax.rem(me + k, groups) for k in range(1, groups)]
    barrier = pltpu.get_barrier_semaphore()
    for other in subs_to:
        pl.semaphore_signal(barrier, inc=1, device_id=(other, me), device_id_type=MESH)
    for other in groups_to:
        pl.semaphore_signal(barrier, inc=1, device_id=(sub, other), device_id_type=MESH)
    pl.semaphore_wait(barrier, subs + groups - 2)

    z_copies = []
    for i, other in enumerate(subs_to):
        copy = pltpu.make_async_remote_copy(
            src_ref=ends, dst_ref=everyone.at[sub], send_sem=z_send.at[i], recv_sem=z_recv.at[i],
            device_id=(other, me), device_id_type=MESH,
        )
        copy.start()
        z_copies.append(copy)
    copies = []
    for i, other in enumerate(groups_to):
        copy = pltpu.make_async_remote_copy(
            src_ref=packed.at[other], dst_ref=landed.at[me],
            send_sem=p_send.at[i], recv_sem=p_recv.at[i],
            device_id=(sub, other), device_id_type=MESH,
        )
        copy.start()
        copies.append(copy)
    own = pltpu.make_async_copy(packed.at[me], landed.at[me], own_sem.at[0])
    own.start()
    everyone[sub] = ends[...]
    for copy in z_copies:
        copy.wait()

    base = 2 * fields * wide
    for f in range(fields):
        for t in range(wide):
            def influence(s, e, w):
                line = everyone[s, base + t, pl.ds(f * 4 + e * 2 + w, 1), :]
                return jnp.broadcast_to(line, (ROWS, LANES))

            def slope(s, e):
                return everyone[s, (e * fields + f) * wide + t]

            zero = jnp.zeros((ROWS, LANES), F32)
            ratio, reduced = zero, zero
            ratios, reduceds = [], []
            for k in range(subs - 1):
                low = influence(k, 1, 0)
                middle = influence(k, 1, 1) - influence(k + 1, 0, 0)
                up = -influence(k + 1, 0, 1)
                right = slope(k + 1, 0) - slope(k, 1)
                pivot = middle - low * ratio
                reduced = (right - low * reduced) / pivot
                ratio = up / pivot
                ratios.append(ratio)
                reduceds.append(reduced)
            later = zero
            lower_value, upper_value = zero, zero
            for k in range(subs - 2, -1, -1):
                later = reduceds[k] - ratios[k] * later
                lower_value = jnp.where(sub == k + 1, later, lower_value)
                upper_value = jnp.where(sub == k, later, upper_value)
            values[f * wide + t] = lower_value
            values[(fields + f) * wide + t] = upper_value

    for i, other in enumerate(groups_to):
        copy = pltpu.make_async_remote_copy(
            src_ref=values, dst_ref=values_landed.at[me],
            send_sem=u_send.at[i], recv_sem=u_recv.at[i],
            device_id=(sub, other), device_id_type=MESH,
        )
        copy.start()
        copies.append(copy)
    own_values = pltpu.make_async_copy(values, values_landed.at[me], own_sem.at[1])
    own_values.start()
    own.wait()
    own_values.wait()
    for copy in copies:
        copy.wait()


def finish_kernel(dims, landed, values, cols, out):
    fields, degrees, group = dims
    tiles = degrees // LANES
    half = tiles // 2
    wide = tiles + half
    row, lane = grid_iotas()
    is_even = (row & 1) == 0
    count = fields * group * tiles
    left = landed[0, count]
    m = landed[0, count + 1].astype(jnp.int32)
    back_index = (lane + m) & (LANES - 1)
    for f in range(fields):
        for p in range(group):
            k = f * group + p
            pieces = [landed[0, k * tiles + t] for t in range(tiles)]
            first = lane_gather(pieces[0], back_index)
            second = lane_gather(pieces[1], back_index)
            spare = lane_gather(left, jnp.full((ROWS, LANES), k, jnp.int32))
            even = [
                jnp.where(lane >= m, pieces[0], 0.0),
                jnp.where(lane + LANES >= m, pieces[1], 0.0),
                pieces[2],
                pieces[3],
            ]
            odd = [None] * half
            moved = [first, jnp.where(lane + m < 2 * LANES, first, second)]
            for t in range(half):
                degree = lane + (half + t) * LANES
                odd[t] = jnp.where(
                    degree >= degrees - m,
                    moved[t],
                    jnp.where(degree == degrees - 1 - m, spare, 0.0),
                )
            for t in range(tiles):
                at = pl.ds(t * LANES, LANES)
                low = jnp.broadcast_to(cols[0, f, pl.ds(p, 1), at], (ROWS, LANES))
                top = jnp.broadcast_to(cols[1, f, pl.ds(p, 1), at], (ROWS, LANES))
                e = even[t] + values[0, f * wide + t] * low
                e = e + values[0, (fields + f) * wide + t] * top
                o = jnp.zeros((ROWS, LANES), F32)
                if t >= half:
                    spot = tiles + t - half
                    o = odd[t - half] + values[0, f * wide + spot] * low
                    o = o + values[0, (fields + f) * wide + spot] * top
                out[f, p, 0, :, at] = jnp.where(is_even, e, pltpu.roll(o, 1, 0))
                out[f, p, 1, :, at] = jnp.where(is_even, pltpu.roll(e, ROWS - 1, 0), o)


def body(forcing, slot_wavenumber, inverse, edge_weights):
    fields, points, halves, slots, degrees = forcing.shape
    subs, groups = lax.axis_size("sub"), lax.axis_size("ma")
    group = points // groups
    tiles = degrees // LANES
    half = tiles // 2
    wide = tiles + half
    assert halves == 2 and slots == ROWS and tiles == 4
    count = fields * group * tiles + 2
    end_count = 2 * fields * wide + wide
    value_count = 2 * fields * wide
    shape = jax.ShapeDtypeStruct
    packed, ends, cols = pl.pallas_call(
        functools.partial(solve_kernel, (fields, points, degrees, group)),
        grid=(groups,),
        in_specs=[
            pl.BlockSpec(memory_space=pltpu.SMEM),
            pl.BlockSpec(memory_space=pltpu.SMEM),
            pl.BlockSpec((fields, points, halves, slots, degrees), lambda g: (0, 0, 0, 0, 0)),
            pl.BlockSpec(
                (1, fields, group, points // ROWS, ROWS, degrees), lambda g: (0, 0, g, 0, 0, 0)
            ),
        ],
        out_specs=[
            pl.BlockSpec((1, count, ROWS, LANES), lambda g: (g, 0, 0, 0)),
            pl.BlockSpec((end_count, ROWS, LANES), lambda g: (0, 0, 0)),
            pl.BlockSpec((2, fields, group, degrees), lambda g: (0, 0, 0, 0)),
        ],
        out_shape=[
            shape((groups, count, ROWS, LANES), F32),
            shape((end_count, ROWS, LANES), F32),
            shape((2, fields, group, degrees), F32),
        ],
        scratch_shapes=[
            pltpu.VMEM((fields, points, tiles, ROWS, LANES), F32),
            pltpu.VMEM((fields, points, half, ROWS, LANES), F32),
            pltpu.VMEM((group, wide, ROWS, LANES), F32),
            pltpu.VMEM((2, fields, 2, tiles, ROWS, LANES), F32),
        ],
        compiler_params=pltpu.CompilerParams(vmem_limit_bytes=40 * 1024 * 1024),
    )(
        slot_wavenumber,
        edge_weights,
        forcing,
        inverse.reshape(1, fields, points, points // ROWS, ROWS, degrees),
    )

    landed, values = pl.pallas_call(
        functools.partial(exchange_kernel, (fields, wide, subs, groups)),
        in_specs=[
            pl.BlockSpec(memory_space=pl.ANY),
            pl.BlockSpec(memory_space=pltpu.VMEM),
        ],
        out_specs=[pl.BlockSpec(memory_space=pl.ANY), pl.BlockSpec(memory_space=pl.ANY)],
        out_shape=[
            shape((groups, count, ROWS, LANES), F32),
            shape((groups, value_count, ROWS, LANES), F32),
        ],
        scratch_shapes=[
            pltpu.VMEM((subs, end_count, ROWS, LANES), F32),
            pltpu.VMEM((value_count, ROWS, LANES), F32),
            pltpu.SemaphoreType.DMA((subs - 1,)),
            pltpu.SemaphoreType.DMA((subs - 1,)),
            pltpu.SemaphoreType.DMA((groups - 1,)),
            pltpu.SemaphoreType.DMA((groups - 1,)),
            pltpu.SemaphoreType.DMA((groups - 1,)),
            pltpu.SemaphoreType.DMA((groups - 1,)),
            pltpu.SemaphoreType.DMA((2,)),
        ],
        compiler_params=pltpu.CompilerParams(collective_id=0, has_side_effects=True),
    )(packed, ends)

    return pl.pallas_call(
        functools.partial(finish_kernel, (fields, degrees, group)),
        grid=(groups,),
        in_specs=[
            pl.BlockSpec((1, count, ROWS, LANES), lambda d: (d, 0, 0, 0)),
            pl.BlockSpec((1, value_count, ROWS, LANES), lambda d: (d, 0, 0, 0)),
            pl.BlockSpec((2, fields, group, degrees), lambda d: (0, 0, 0, 0)),
        ],
        out_specs=pl.BlockSpec(
            (fields, group, halves, slots, degrees), lambda d: (0, 0, 0, d, 0)
        ),
        out_shape=shape((fields, group, halves, slots * groups, degrees), F32),
        compiler_params=pltpu.CompilerParams(vmem_limit_bytes=24 * 1024 * 1024),
    )(landed, values, cols)


def solution(mesh):
    return jax.shard_map(
        body,
        mesh=mesh,
        in_specs=(
            P(None, "sub", None, "ma", None),
            P("ma"),
            P("sub", None, None, None, None),
            P("sub", None, None),
        ),
        out_specs=P(None, ("sub", "ma"), None, None, None),
        check_vma=False,
    )
```

```python
import functools

import jax
import jax.numpy as jnp
from jax import lax
from jax.experimental import pallas as pl
from jax.experimental.pallas import tpu as pltpu
from jax.sharding import PartitionSpec as P

LANES = 128
ROWS = 8
F32 = jnp.float32
MESH = pl.DeviceIdType.MESH
FIRST = 2
VMEM_BYTES = 60 * 1024 * 1024
EARLY = 2


def grid_iotas():
    row = lax.broadcasted_iota(jnp.int32, (ROWS, LANES), 0)
    lane = lax.broadcasted_iota(jnp.int32, (ROWS, LANES), 1)
    return row, lane


def lane_gather(values, index):
    return jnp.take_along_axis(values, index, axis=1, mode="promise_in_bounds")


def solve_kernel(
    dims, slot, edge, forcing, inverse, landed, values_landed, cols,
    raw, blocks_in, even_src, odd_src, part, weighed, packed, ends, everyone, values,
    raw_sem, in_sem, z_send, z_recv, p_send, p_recv, u_send, u_recv, own_sem,
):
    fields, points, degrees, group, subs, groups = dims
    tiles = degrees // LANES
    half = tiles // 2
    wide = tiles + half
    blocks = points // ROWS
    base = 2 * fields * wide
    sub = lax.axis_index("sub")
    me = lax.axis_index("ma")
    row, lane = grid_iotas()
    is_even = (row & 1) == 0

    def target(i):
        return lax.rem(me + lax.rem(i + FIRST, groups), groups)

    def fetch(i):
        return pltpu.make_async_copy(
            inverse.at[0, :, pl.ds(target(i) * group, group)], blocks_in.at[i], in_sem.at[i]
        )

    def send(i):
        return pltpu.make_async_remote_copy(
            src_ref=packed.at[i], dst_ref=landed.at[me],
            send_sem=p_send.at[i], recv_sem=p_recv.at[i],
            device_id=(sub, target(i)), device_id_type=MESH,
        )

    def send_values(i):
        return pltpu.make_async_remote_copy(
            src_ref=values, dst_ref=values_landed.at[me],
            send_sem=u_send.at[i], recv_sem=u_recv.at[i],
            device_id=(sub, target(i)), device_id_type=MESH,
        )

    others = [i for i in range(groups) if (i + FIRST) % groups != 0]
    mine = groups - FIRST
    load = pltpu.make_async_copy(forcing, raw, raw_sem.at[0])
    load.start()
    for i in range(groups):
        fetch(i).start()
    barrier = pltpu.get_barrier_semaphore()
    subs_to = [lax.rem(sub + k, subs) for k in range(1, subs)]
    for other in subs_to:
        pl.semaphore_signal(barrier, inc=1, device_id=(other, me), device_id_type=MESH)
    for i in others:
        pl.semaphore_signal(barrier, inc=1, device_id=(sub, target(i)), device_id_type=MESH)

    m = jnp.zeros((ROWS, LANES), jnp.int32)
    for j in range(ROWS // 2):
        m = jnp.where((row >> 1) == j, slot[2 * j], m)
    load.wait()

    def prepare(q, _):
        inside = jnp.where((q > 0) & (q < points - 1), 1.0, 0.0).astype(F32)
        for f in range(fields):
            for t in range(tiles):
                at = pl.ds(t * LANES, LANES)
                a = raw[f, q, 0, :, at] * inside
                b = raw[f, q, 1, :, at] * inside
                degree = lane + t * LANES
                mixed = jnp.where(is_even, a, pltpu.roll(b, 1, 0))
                even_src[f, q, t] = jnp.where(degree >= m, mixed, 0.0)
                if t >= half:
                    mixed = jnp.where(is_even, pltpu.roll(a, ROWS - 1, 0), b)
                    odd_src[f, q, t - half] = jnp.where(degree >= degrees - 1 - m, mixed, 0.0)
        return 0

    lax.fori_loop(0, points, prepare, 0)
    pl.semaphore_wait(barrier, subs + groups - 2)

    shift_index = (lane - m) & (LANES - 1)
    left_index = (degrees - 1 - m) & (LANES - 1)

    def solve_group(i):
        left = jnp.zeros((ROWS, LANES), F32)
        for f in range(fields):
            for t in range(tiles):
                at = pl.ds(t * LANES, LANES)
                both = t >= half

                def step(block, sums, f=f, t=t, at=at, both=both):
                    sums = list(sums)
                    for r in range(ROWS):
                        q = block * ROWS + r
                        even = even_src[f, q, t]
                        odd = odd_src[f, q, t - half] if both else None
                        for p in range(group):
                            line = blocks_in[i, f, p, block, pl.ds(r, 1), at]
                            entry = jnp.broadcast_to(line, (ROWS, LANES))
                            sums[p] += entry * even
                            if both:
                                sums[group + p] += entry * odd
                    return tuple(sums)

                count = group * (2 if both else 1)
                start = tuple(jnp.zeros((ROWS, LANES), F32) for _ in range(count))
                sums = lax.fori_loop(0, blocks, step, start)
                for p in range(group):
                    part[p, t] = sums[p]
                    if both:
                        part[p, tiles + t - half] = sums[group + p]
            for p in range(group):
                k = f * group + p
                near, far = part[p, tiles], part[p, tiles + 1]
                near_moved = lane_gather(near, shift_index)
                far_moved = lane_gather(far, shift_index)
                packed[i, k * tiles] = jnp.where(
                    lane >= m, part[p, 0], jnp.where(lane - m >= -LANES, far_moved, near_moved)
                )
                packed[i, k * tiles + 1] = jnp.where(lane + LANES >= m, part[p, 1], far_moved)
                packed[i, k * tiles + 2] = part[p, 2]
                packed[i, k * tiles + 3] = part[p, 3]
                spare = jnp.where(
                    m < LANES, lane_gather(far, left_index), lane_gather(near, left_index)
                )
                left = jnp.where(lane == k, spare, left)
        packed[i, fields * group * tiles] = left
        packed[i, fields * group * tiles + 1] = m.astype(F32)

    own = pltpu.make_async_copy(packed.at[mine], landed.at[me], own_sem.at[0])

    def early(i, _):
        fetch(i).wait()
        solve_group(i)
        send(i).start()
        return 0

    lax.fori_loop(0, EARLY, early, 0)
    for i in range(EARLY, groups):
        fetch(i).wait()

    def weigh(block, _):
        for f in range(fields):
            def add(i, sums, f=f):
                sums = list(sums)
                for p in range(group):
                    low = edge[0, 0, target(i) * group + p]
                    top = edge[0, 1, target(i) * group + p]
                    for t in range(tiles):
                        entry = blocks_in[i, f, p, block, :, pl.ds(t * LANES, LANES)]
                        sums[t] += low * entry
                        sums[tiles + t] += top * entry
                return tuple(sums)

            start = tuple(jnp.zeros((ROWS, LANES), F32) for _ in range(2 * tiles))
            sums = lax.fori_loop(0, groups, add, start)
            for t in range(tiles):
                weighed[0, f, block, t] = sums[t]
                weighed[1, f, block, t] = sums[tiles + t]
        return 0

    lax.fori_loop(0, blocks, weigh, 0)
    for f in range(fields):
        def slope_step(block, sums, f=f):
            sums = list(sums)
            for r in range(ROWS):
                q = block * ROWS + r
                for e in range(2):
                    for t in range(tiles):
                        line = weighed[e, f, block, t, pl.ds(r, 1), :]
                        entry = jnp.broadcast_to(line, (ROWS, LANES))
                        sums[e * wide + t] += entry * even_src[f, q, t]
                        if t >= half:
                            sums[e * wide + t + half] += entry * odd_src[f, q, t - half]
            return tuple(sums)

        start = tuple(jnp.zeros((ROWS, LANES), F32) for _ in range(2 * wide))
        sums = lax.fori_loop(0, blocks, slope_step, start)
        for e in range(2):
            for t in range(wide):
                ends[(e * fields + f) * wide + t] = sums[e * wide + t]
            for w in range(2):
                for t in range(wide):
                    source = t if t < tiles else t - half
                    line = weighed[e, f, w * (blocks - 1), source, pl.ds(w * (ROWS - 1), 1), :]
                    ends[base + t, pl.ds(f * 4 + e * 2 + w, 1), :] = line

    z_copies = []
    for i, other in enumerate(subs_to):
        copy = pltpu.make_async_remote_copy(
            src_ref=ends, dst_ref=everyone.at[sub], send_sem=z_send.at[i], recv_sem=z_recv.at[i],
            device_id=(other, me), device_id_type=MESH,
        )
        copy.start()
        z_copies.append(copy)
    everyone[sub] = ends[...]

    def late(i, _):
        solve_group(i)

        @pl.when(i != mine)
        def _():
            send(i).start()

        @pl.when(i == mine)
        def _():
            own.start()

        return 0

    lax.fori_loop(EARLY, groups, late, 0)
    for f in range(fields):
        for p in range(group):
            cols[0, f, pl.ds(p, 1), :] = blocks_in[mine, f, p, 0, pl.ds(0, 1), :]
            cols[1, f, pl.ds(p, 1), :] = blocks_in[mine, f, p, blocks - 1, pl.ds(ROWS - 1, 1), :]
    for copy in z_copies:
        copy.wait()

    for f in range(fields):
        for t in range(wide):
            def influence(s, e, w):
                line = everyone[s, base + t, pl.ds(f * 4 + e * 2 + w, 1), :]
                return jnp.broadcast_to(line, (ROWS, LANES))

            def slope(s, e):
                return everyone[s, (e * fields + f) * wide + t]

            zero = jnp.zeros((ROWS, LANES), F32)
            ratio, reduced = zero, zero
            ratios, reduceds = [], []
            for k in range(subs - 1):
                low = influence(k, 1, 0)
                middle = influence(k, 1, 1) - influence(k + 1, 0, 0)
                up = -influence(k + 1, 0, 1)
                right = slope(k + 1, 0) - slope(k, 1)
                pivot = middle - low * ratio
                reduced = (right - low * reduced) / pivot
                ratio = up / pivot
                ratios.append(ratio)
                reduceds.append(reduced)
            later = zero
            lower_value, upper_value = zero, zero
            for k in range(subs - 2, -1, -1):
                later = reduceds[k] - ratios[k] * later
                lower_value = jnp.where(sub == k + 1, later, lower_value)
                upper_value = jnp.where(sub == k, later, upper_value)
            values[f * wide + t] = lower_value
            values[(fields + f) * wide + t] = upper_value

    for i in others:
        send_values(i).start()
    own_values = pltpu.make_async_copy(values, values_landed.at[me], own_sem.at[1])
    own_values.start()
    own.wait()
    own_values.wait()
    for i in others:
        send(i).wait()
        send_values(i).wait()


def finish_kernel(dims, landed, values, cols, out):
    fields, degrees, group = dims
    tiles = degrees // LANES
    half = tiles // 2
    wide = tiles + half
    row, lane = grid_iotas()
    is_even = (row & 1) == 0
    count = fields * group * tiles
    left = landed[0, count]
    m = landed[0, count + 1].astype(jnp.int32)
    back_index = (lane + m) & (LANES - 1)
    for f in range(fields):
        for p in range(group):
            k = f * group + p
            pieces = [landed[0, k * tiles + t] for t in range(tiles)]
            first = lane_gather(pieces[0], back_index)
            second = lane_gather(pieces[1], back_index)
            spare = lane_gather(left, jnp.full((ROWS, LANES), k, jnp.int32))
            even = [
                jnp.where(lane >= m, pieces[0], 0.0),
                jnp.where(lane + LANES >= m, pieces[1], 0.0),
                pieces[2],
                pieces[3],
            ]
            odd = [None] * half
            moved = [first, jnp.where(lane + m < 2 * LANES, first, second)]
            for t in range(half):
                degree = lane + (half + t) * LANES
                odd[t] = jnp.where(
                    degree >= degrees - m,
                    moved[t],
                    jnp.where(degree == degrees - 1 - m, spare, 0.0),
                )
            for t in range(tiles):
                at = pl.ds(t * LANES, LANES)
                low = jnp.broadcast_to(cols[0, f, pl.ds(p, 1), at], (ROWS, LANES))
                top = jnp.broadcast_to(cols[1, f, pl.ds(p, 1), at], (ROWS, LANES))
                e = even[t] + values[0, f * wide + t] * low
                e = e + values[0, (fields + f) * wide + t] * top
                o = jnp.zeros((ROWS, LANES), F32)
                if t >= half:
                    spot = tiles + t - half
                    o = odd[t - half] + values[0, f * wide + spot] * low
                    o = o + values[0, (fields + f) * wide + spot] * top
                out[f, p, 0, :, at] = jnp.where(is_even, e, pltpu.roll(o, 1, 0))
                out[f, p, 1, :, at] = jnp.where(is_even, pltpu.roll(e, ROWS - 1, 0), o)


def body(forcing, slot_wavenumber, inverse, edge_weights):
    fields, points, halves, slots, degrees = forcing.shape
    subs, groups = lax.axis_size("sub"), lax.axis_size("ma")
    group = points // groups
    tiles = degrees // LANES
    half = tiles // 2
    wide = tiles + half
    assert halves == 2 and slots == ROWS and tiles == 4
    count = fields * group * tiles + 2
    end_count = 2 * fields * wide + wide
    value_count = 2 * fields * wide
    shape = jax.ShapeDtypeStruct
    blocks = points // ROWS
    landed, values, cols = pl.pallas_call(
        functools.partial(solve_kernel, (fields, points, degrees, group, subs, groups)),
        in_specs=[
            pl.BlockSpec(memory_space=pltpu.SMEM),
            pl.BlockSpec(memory_space=pltpu.SMEM),
            pl.BlockSpec(memory_space=pl.ANY),
            pl.BlockSpec(memory_space=pl.ANY),
        ],
        out_specs=[
            pl.BlockSpec(memory_space=pl.ANY),
            pl.BlockSpec(memory_space=pl.ANY),
            pl.BlockSpec(memory_space=pltpu.VMEM),
        ],
        out_shape=[
            shape((groups, count, ROWS, LANES), F32),
            shape((groups, value_count, ROWS, LANES), F32),
            shape((2, fields, group, degrees), F32),
        ],
        scratch_shapes=[
            pltpu.VMEM((fields, points, halves, slots, degrees), F32),
            pltpu.VMEM((groups, fields, group, blocks, ROWS, degrees), F32),
            pltpu.VMEM((fields, points, tiles, ROWS, LANES), F32),
            pltpu.VMEM((fields, points, half, ROWS, LANES), F32),
            pltpu.VMEM((group, wide, ROWS, LANES), F32),
            pltpu.VMEM((2, fields, blocks, tiles, ROWS, LANES), F32),
            pltpu.VMEM((groups, count, ROWS, LANES), F32),
            pltpu.VMEM((end_count, ROWS, LANES), F32),
            pltpu.VMEM((subs, end_count, ROWS, LANES), F32),
            pltpu.VMEM((value_count, ROWS, LANES), F32),
            pltpu.SemaphoreType.DMA((1,)),
            pltpu.SemaphoreType.DMA((groups,)),
            pltpu.SemaphoreType.DMA((subs - 1,)),
            pltpu.SemaphoreType.DMA((subs - 1,)),
            pltpu.SemaphoreType.DMA((groups,)),
            pltpu.SemaphoreType.DMA((groups,)),
            pltpu.SemaphoreType.DMA((groups,)),
            pltpu.SemaphoreType.DMA((groups,)),
            pltpu.SemaphoreType.DMA((2,)),
        ],
        compiler_params=pltpu.CompilerParams(
            collective_id=0, has_side_effects=True, vmem_limit_bytes=VMEM_BYTES
        ),
    )(
        slot_wavenumber,
        edge_weights,
        forcing,
        inverse.reshape(1, fields, points, blocks, ROWS, degrees),
    )

    return pl.pallas_call(
        functools.partial(finish_kernel, (fields, degrees, group)),
        grid=(groups,),
        in_specs=[
            pl.BlockSpec((1, count, ROWS, LANES), lambda d: (d, 0, 0, 0)),
            pl.BlockSpec((1, value_count, ROWS, LANES), lambda d: (d, 0, 0, 0)),
            pl.BlockSpec((2, fields, group, degrees), lambda d: (0, 0, 0, 0)),
        ],
        out_specs=pl.BlockSpec(
            (fields, group, halves, slots, degrees), lambda d: (0, 0, 0, d, 0)
        ),
        out_shape=shape((fields, group, halves, slots * groups, degrees), F32),
        compiler_params=pltpu.CompilerParams(vmem_limit_bytes=VMEM_BYTES),
    )(landed, values, cols)


def solution(mesh):
    return jax.shard_map(
        body,
        mesh=mesh,
        in_specs=(
            P(None, "sub", None, "ma", None),
            P("ma"),
            P("sub", None, None, None, None),
            P("sub", None, None),
        ),
        out_specs=P(None, ("sub", "ma"), None, None, None),
        check_vma=False,
    )
```

```python
import functools

import jax
import jax.numpy as jnp
from jax import lax
from jax.experimental import pallas as pl
from jax.experimental.pallas import tpu as pltpu
from jax.sharding import PartitionSpec as P

LANES = 128
ROWS = 8
F32 = jnp.float32
MESH = pl.DeviceIdType.MESH
FIRST = 2
VMEM_BYTES = 60 * 1024 * 1024
EARLY = 2


def grid_iotas():
    row = lax.broadcasted_iota(jnp.int32, (ROWS, LANES), 0)
    lane = lax.broadcasted_iota(jnp.int32, (ROWS, LANES), 1)
    return row, lane


def lane_gather(values, index):
    return jnp.take_along_axis(values, index, axis=1, mode="promise_in_bounds")


def solve_kernel(
    dims, slot, edge, forcing, inverse, landed, values_landed, cols,
    raw, blocks_in, even_src, odd_src, part, weighed, packed, ends, everyone, values,
    raw_sem, in_sem, z_send, z_recv, p_send, p_recv, u_send, u_recv, f_send, f_recv, own_sem,
):
    fields, points, degrees, group, subs, groups = dims
    tiles = degrees // LANES
    half = tiles // 2
    wide = tiles + half
    blocks = points // ROWS
    base = 2 * fields * wide
    sub = lax.axis_index("sub")
    me = lax.axis_index("ma")
    row, lane = grid_iotas()
    is_even = (row & 1) == 0

    def target(i):
        return lax.rem(me + lax.rem(i + FIRST, groups), groups)

    def fetch(i):
        return pltpu.make_async_copy(
            inverse.at[0, :, pl.ds(target(i) * group, group)], blocks_in.at[i], in_sem.at[i]
        )

    def send(i):
        return pltpu.make_async_remote_copy(
            src_ref=packed.at[i], dst_ref=landed.at[me],
            send_sem=p_send.at[i], recv_sem=p_recv.at[i],
            device_id=(sub, target(i)), device_id_type=MESH,
        )

    pair = me + 1 - 2 * lax.rem(me, 2)
    senders = [lax.rem(me + groups - k, groups) for k in range(0, groups, 2)]

    def send_values(k):
        to = pair if k == 0 else lax.rem(me + k, groups)
        return pltpu.make_async_remote_copy(
            src_ref=values, dst_ref=values_landed.at[me],
            send_sem=u_send.at[k // 2], recv_sem=u_recv.at[k // 2],
            device_id=(sub, to), device_id_type=MESH,
        )

    def forward(k):
        block = values_landed.at[senders[k // 2]]
        return pltpu.make_async_remote_copy(
            src_ref=block, dst_ref=block,
            send_sem=f_send.at[k // 2], recv_sem=f_recv.at[k // 2],
            device_id=(sub, pair), device_id_type=MESH,
        )

    others = [i for i in range(groups) if (i + FIRST) % groups != 0]
    mine = groups - FIRST
    load = pltpu.make_async_copy(forcing, raw, raw_sem.at[0])
    load.start()
    fetch(0).start()
    barrier = pltpu.get_barrier_semaphore()
    subs_to = [lax.rem(sub + k, subs) for k in range(1, subs)]
    for other in subs_to:
        pl.semaphore_signal(barrier, inc=1, device_id=(other, me), device_id_type=MESH)
    for i in others:
        pl.semaphore_signal(barrier, inc=1, device_id=(sub, target(i)), device_id_type=MESH)

    m = jnp.zeros((ROWS, LANES), jnp.int32)
    for j in range(ROWS // 2):
        m = jnp.where((row >> 1) == j, slot[2 * j], m)
    load.wait()
    for i in range(1, groups):
        fetch(i).start()

    def prepare(q, _):
        inside = jnp.where((q > 0) & (q < points - 1), 1.0, 0.0).astype(F32)
        for f in range(fields):
            for t in range(tiles):
                at = pl.ds(t * LANES, LANES)
                a = raw[f, q, 0, :, at] * inside
                b = raw[f, q, 1, :, at] * inside
                degree = lane + t * LANES
                mixed = jnp.where(is_even, a, pltpu.roll(b, 1, 0))
                even_src[f, q, t] = jnp.where(degree >= m, mixed, 0.0)
                if t >= half:
                    mixed = jnp.where(is_even, pltpu.roll(a, ROWS - 1, 0), b)
                    odd_src[f, q, t - half] = jnp.where(degree >= degrees - 1 - m, mixed, 0.0)
        return 0

    lax.fori_loop(0, points, prepare, 0)
    pl.semaphore_wait(barrier, subs + groups - 2)

    shift_index = (lane - m) & (LANES - 1)
    left_index = (degrees - 1 - m) & (LANES - 1)

    def solve_group(i):
        left = jnp.zeros((ROWS, LANES), F32)
        for f in range(fields):
            for t in range(tiles):
                at = pl.ds(t * LANES, LANES)
                both = t >= half

                def step(block, sums, f=f, t=t, at=at, both=both):
                    sums = list(sums)
                    for r in range(ROWS):
                        q = block * ROWS + r
                        even = even_src[f, q, t]
                        odd = odd_src[f, q, t - half] if both else None
                        for p in range(group):
                            line = blocks_in[i, f, p, block, pl.ds(r, 1), at]
                            entry = jnp.broadcast_to(line, (ROWS, LANES))
                            sums[p] += entry * even
                            if both:
                                sums[group + p] += entry * odd
                    return tuple(sums)

                count = group * (2 if both else 1)
                start = tuple(jnp.zeros((ROWS, LANES), F32) for _ in range(count))
                sums = lax.fori_loop(0, blocks, step, start)
                for p in range(group):
                    part[p, t] = sums[p]
                    if both:
                        part[p, tiles + t - half] = sums[group + p]
            for p in range(group):
                k = f * group + p
                near, far = part[p, tiles], part[p, tiles + 1]
                near_moved = lane_gather(near, shift_index)
                far_moved = lane_gather(far, shift_index)
                packed[i, k * tiles] = jnp.where(
                    lane >= m, part[p, 0], jnp.where(lane - m >= -LANES, far_moved, near_moved)
                )
                packed[i, k * tiles + 1] = jnp.where(lane + LANES >= m, part[p, 1], far_moved)
                packed[i, k * tiles + 2] = part[p, 2]
                packed[i, k * tiles + 3] = part[p, 3]
                spare = jnp.where(
                    m < LANES, lane_gather(far, left_index), lane_gather(near, left_index)
                )
                left = jnp.where(lane == k, spare, left)
        packed[i, fields * group * tiles] = left
        packed[i, fields * group * tiles + 1] = m.astype(F32)

    own = pltpu.make_async_copy(packed.at[mine], landed.at[me], own_sem.at[0])

    def early(i, _):
        fetch(i).wait()
        solve_group(i)
        send(i).start()
        return 0

    lax.fori_loop(0, EARLY, early, 0)
    for i in range(EARLY, groups):
        fetch(i).wait()

    def weigh(block, _):
        for f in range(fields):
            def add(i, sums, f=f):
                sums = list(sums)
                for p in range(group):
                    low = edge[0, 0, target(i) * group + p]
                    top = edge[0, 1, target(i) * group + p]
                    for t in range(tiles):
                        entry = blocks_in[i, f, p, block, :, pl.ds(t * LANES, LANES)]
                        sums[t] += low * entry
                        sums[tiles + t] += top * entry
                return tuple(sums)

            start = tuple(jnp.zeros((ROWS, LANES), F32) for _ in range(2 * tiles))
            sums = lax.fori_loop(0, groups, add, start)
            for t in range(tiles):
                weighed[0, f, block, t] = sums[t]
                weighed[1, f, block, t] = sums[tiles + t]
        return 0

    lax.fori_loop(0, blocks, weigh, 0)
    for f in range(fields):
        def slope_step(block, sums, f=f):
            sums = list(sums)
            for r in range(ROWS):
                q = block * ROWS + r
                for e in range(2):
                    for t in range(tiles):
                        line = weighed[e, f, block, t, pl.ds(r, 1), :]
                        entry = jnp.broadcast_to(line, (ROWS, LANES))
                        sums[e * wide + t] += entry * even_src[f, q, t]
                        if t >= half:
                            sums[e * wide + t + half] += entry * odd_src[f, q, t - half]
            return tuple(sums)

        start = tuple(jnp.zeros((ROWS, LANES), F32) for _ in range(2 * wide))
        sums = lax.fori_loop(0, blocks, slope_step, start)
        for e in range(2):
            for t in range(wide):
                ends[(e * fields + f) * wide + t] = sums[e * wide + t]
            for w in range(2):
                for t in range(wide):
                    source = t if t < tiles else t - half
                    line = weighed[e, f, w * (blocks - 1), source, pl.ds(w * (ROWS - 1), 1), :]
                    ends[base + t, pl.ds(f * 4 + e * 2 + w, 1), :] = line

    z_copies = []
    for i, other in enumerate(subs_to):
        copy = pltpu.make_async_remote_copy(
            src_ref=ends, dst_ref=everyone.at[sub], send_sem=z_send.at[i], recv_sem=z_recv.at[i],
            device_id=(other, me), device_id_type=MESH,
        )
        copy.start()
        z_copies.append(copy)
    everyone[sub] = ends[...]

    def late(i, _):
        solve_group(i)

        @pl.when(i != mine)
        def _():
            send(i).start()

        @pl.when(i == mine)
        def _():
            own.start()

        return 0

    lax.fori_loop(EARLY, groups, late, 0)
    for f in range(fields):
        for p in range(group):
            cols[0, f, pl.ds(p, 1), :] = blocks_in[mine, f, p, 0, pl.ds(0, 1), :]
            cols[1, f, pl.ds(p, 1), :] = blocks_in[mine, f, p, blocks - 1, pl.ds(ROWS - 1, 1), :]
    for copy in z_copies:
        copy.wait()

    for f in range(fields):
        for t in range(wide):
            def influence(s, e, w):
                line = everyone[s, base + t, pl.ds(f * 4 + e * 2 + w, 1), :]
                return jnp.broadcast_to(line, (ROWS, LANES))

            def slope(s, e):
                return everyone[s, (e * fields + f) * wide + t]

            zero = jnp.zeros((ROWS, LANES), F32)
            ratio, reduced = zero, zero
            ratios, reduceds = [], []
            for k in range(subs - 1):
                low = influence(k, 1, 0)
                middle = influence(k, 1, 1) - influence(k + 1, 0, 0)
                up = -influence(k + 1, 0, 1)
                right = slope(k + 1, 0) - slope(k, 1)
                pivot = middle - low * ratio
                reduced = (right - low * reduced) / pivot
                ratio = up / pivot
                ratios.append(ratio)
                reduceds.append(reduced)
            later = zero
            lower_value, upper_value = zero, zero
            for k in range(subs - 2, -1, -1):
                later = reduceds[k] - ratios[k] * later
                lower_value = jnp.where(sub == k + 1, later, lower_value)
                upper_value = jnp.where(sub == k, later, upper_value)
            values[f * wide + t] = lower_value
            values[(fields + f) * wide + t] = upper_value

    for k in list(range(2, groups, 2)) + [0]:
        send_values(k).start()
    own_values = pltpu.make_async_copy(values, values_landed.at[me], own_sem.at[1])
    own_values.start()
    for k in range(2, groups, 2):
        send_values(k).wait_recv()
        forward(k).start()
    own.wait()
    own_values.wait()
    for i in others:
        send(i).wait()
    send_values(0).wait()
    for k in range(2, groups, 2):
        send_values(k).wait_send()
        forward(k).wait()


def finish_kernel(
    dims, landed_in, values_in, cols, result, landed, values, out, landed_sem, values_sem, out_sem
):
    fields, degrees, group, groups = dims
    tiles = degrees // LANES
    half = tiles // 2
    wide = tiles + half

    def take(d):
        return pltpu.make_async_copy(landed_in.at[d], landed.at[d], landed_sem.at[d])

    def take_values(d):
        return pltpu.make_async_copy(values_in.at[d], values.at[d], values_sem.at[d])

    def put(d):
        rows = pl.ds(pl.multiple_of(d * ROWS, ROWS), ROWS)
        return pltpu.make_async_copy(out.at[d], result.at[:, :, :, rows, :], out_sem.at[d])

    for d in range(groups):
        take(d).start()
        take_values(d).start()
    row, lane = grid_iotas()
    is_even = (row & 1) == 0

    def unpack(d, _):
        take(d).wait()
        take_values(d).wait()
        count = fields * group * tiles
        left = landed[d, count]
        m = landed[d, count + 1].astype(jnp.int32)
        back_index = (lane + m) & (LANES - 1)
        for f in range(fields):
            for p in range(group):
                k = f * group + p
                pieces = [landed[d, k * tiles + t] for t in range(tiles)]
                first = lane_gather(pieces[0], back_index)
                second = lane_gather(pieces[1], back_index)
                spare = lane_gather(left, jnp.full((ROWS, LANES), k, jnp.int32))
                even = [
                    jnp.where(lane >= m, pieces[0], 0.0),
                    jnp.where(lane + LANES >= m, pieces[1], 0.0),
                    pieces[2],
                    pieces[3],
                ]
                odd = [None] * half
                moved = [first, jnp.where(lane + m < 2 * LANES, first, second)]
                for t in range(half):
                    degree = lane + (half + t) * LANES
                    odd[t] = jnp.where(
                        degree >= degrees - m,
                        moved[t],
                        jnp.where(degree == degrees - 1 - m, spare, 0.0),
                    )
                for t in range(tiles):
                    at = pl.ds(t * LANES, LANES)
                    low = jnp.broadcast_to(cols[0, f, pl.ds(p, 1), at], (ROWS, LANES))
                    top = jnp.broadcast_to(cols[1, f, pl.ds(p, 1), at], (ROWS, LANES))
                    e = even[t] + values[d, f * wide + t] * low
                    e = e + values[d, (fields + f) * wide + t] * top
                    o = jnp.zeros((ROWS, LANES), F32)
                    if t >= half:
                        spot = tiles + t - half
                        o = odd[t - half] + values[d, f * wide + spot] * low
                        o = o + values[d, (fields + f) * wide + spot] * top
                    out[d, f, p, 0, :, at] = jnp.where(is_even, e, pltpu.roll(o, 1, 0))
                    out[d, f, p, 1, :, at] = jnp.where(is_even, pltpu.roll(e, ROWS - 1, 0), o)
        put(d).start()
        return 0

    lax.fori_loop(0, groups, unpack, 0)
    for d in range(groups):
        put(d).wait()


def body(forcing, slot_wavenumber, inverse, edge_weights):
    fields, points, halves, slots, degrees = forcing.shape
    subs, groups = lax.axis_size("sub"), lax.axis_size("ma")
    group = points // groups
    tiles = degrees // LANES
    half = tiles // 2
    wide = tiles + half
    assert halves == 2 and slots == ROWS and tiles == 4
    count = fields * group * tiles + 2
    end_count = 2 * fields * wide + wide
    value_count = 2 * fields * wide
    shape = jax.ShapeDtypeStruct
    blocks = points // ROWS
    landed, values, cols = pl.pallas_call(
        functools.partial(solve_kernel, (fields, points, degrees, group, subs, groups)),
        in_specs=[
            pl.BlockSpec(memory_space=pltpu.SMEM),
            pl.BlockSpec(memory_space=pltpu.SMEM),
            pl.BlockSpec(memory_space=pl.ANY),
            pl.BlockSpec(memory_space=pl.ANY),
        ],
        out_specs=[
            pl.BlockSpec(memory_space=pl.ANY),
            pl.BlockSpec(memory_space=pl.ANY),
            pl.BlockSpec(memory_space=pltpu.VMEM),
        ],
        out_shape=[
            shape((groups, count, ROWS, LANES), F32),
            shape((groups, value_count, ROWS, LANES), F32),
            shape((2, fields, group, degrees), F32),
        ],
        scratch_shapes=[
            pltpu.VMEM((fields, points, halves, slots, degrees), F32),
            pltpu.VMEM((groups, fields, group, blocks, ROWS, degrees), F32),
            pltpu.VMEM((fields, points, tiles, ROWS, LANES), F32),
            pltpu.VMEM((fields, points, half, ROWS, LANES), F32),
            pltpu.VMEM((group, wide, ROWS, LANES), F32),
            pltpu.VMEM((2, fields, blocks, tiles, ROWS, LANES), F32),
            pltpu.VMEM((groups, count, ROWS, LANES), F32),
            pltpu.VMEM((end_count, ROWS, LANES), F32),
            pltpu.VMEM((subs, end_count, ROWS, LANES), F32),
            pltpu.VMEM((value_count, ROWS, LANES), F32),
            pltpu.SemaphoreType.DMA((1,)),
            pltpu.SemaphoreType.DMA((groups,)),
            pltpu.SemaphoreType.DMA((subs - 1,)),
            pltpu.SemaphoreType.DMA((subs - 1,)),
            pltpu.SemaphoreType.DMA((groups,)),
            pltpu.SemaphoreType.DMA((groups,)),
            pltpu.SemaphoreType.DMA((groups // 2,)),
            pltpu.SemaphoreType.DMA((groups // 2,)),
            pltpu.SemaphoreType.DMA((groups // 2,)),
            pltpu.SemaphoreType.DMA((groups // 2,)),
            pltpu.SemaphoreType.DMA((2,)),
        ],
        compiler_params=pltpu.CompilerParams(
            collective_id=0, has_side_effects=True, vmem_limit_bytes=VMEM_BYTES
        ),
    )(
        slot_wavenumber,
        edge_weights,
        forcing,
        inverse.reshape(1, fields, points, blocks, ROWS, degrees),
    )

    return pl.pallas_call(
        functools.partial(finish_kernel, (fields, degrees, group, groups)),
        in_specs=[
            pl.BlockSpec(memory_space=pl.ANY),
            pl.BlockSpec(memory_space=pl.ANY),
            pl.BlockSpec(memory_space=pltpu.VMEM),
        ],
        out_specs=pl.BlockSpec(memory_space=pl.ANY),
        out_shape=shape((fields, group, halves, slots * groups, degrees), F32),
        scratch_shapes=[
            pltpu.VMEM((groups, count, ROWS, LANES), F32),
            pltpu.VMEM((groups, value_count, ROWS, LANES), F32),
            pltpu.VMEM((groups, fields, group, halves, slots, degrees), F32),
            pltpu.SemaphoreType.DMA((groups,)),
            pltpu.SemaphoreType.DMA((groups,)),
            pltpu.SemaphoreType.DMA((groups,)),
        ],
        compiler_params=pltpu.CompilerParams(vmem_limit_bytes=VMEM_BYTES),
    )(landed, values, cols)


def solution(mesh):
    return jax.shard_map(
        body,
        mesh=mesh,
        in_specs=(
            P(None, "sub", None, "ma", None),
            P("ma"),
            P("sub", None, None, None, None),
            P("sub", None, None),
        ),
        out_specs=P(None, ("sub", "ma"), None, None, None),
        check_vma=False,
    )
```
